256 devices in a mesh: section: 8 (over z), sp: 32 (over y, x, core).
Axes of the slice: x: 4, y: 4, z: 8, core: 2. Of those that a mesh axis runs over, the one named last changes fastest.
Arguments:
- queries: bfloat16 [8, 2, 6, 512, 32, 128], P('section', None, None, 'sp'), may hold values from -400 to 400
- keys: bfloat16 [8, 2, 6, 512, 4, 128], P('section', None, None, 'sp'), may hold values from -31 to 31
- values: bfloat16 [8, 2, 6, 512, 4, 128], P('section', None, None, 'sp'), may hold values from -6 to 6
- top_grad: bfloat16 [2, 6, 512, 32, 128], P(None, None, 'sp'), may hold values from -6 to 6
- head_live: int32 [32], replicated, may hold values 0 or 1
Outputs:
- input_grad: bfloat16 [8, 2, 6, 512, 32, 128], P('section', None, None, 'sp')
- key_grad: float32 [8, 2, 6, 512, 4, 128], P('section', None, None, 'sp')
- value_grad: float32 [8, 2, 6, 512, 4, 128], P('section', None, None, 'sp')
The draws below stay inside these ranges and needn't reach their ends.
All inputs are finite; a program needn't handle non-finite values.
Results may differ from the reference program's by a relative error of at most 0.01.
Values may be sent and summed in bfloat16 or wider, within the bound.
No kernel may reach another device: no remote copies, remote signals or barrier semaphores. Data moves between devices by JAX's collectives and lax.ppermute only.
A program may use at most 64 MiB of HBM per device.

```python
import jax
import jax.numpy as jnp
from jax import lax

QH = 32
KVH = 4
HD = 128
SPAN = 512
NCH = 6
SEQS = 2
LAYERS = 8


def shared_draw(key):
    folded = jax.random.fold_in(key, 7)
    key_q, key_k = jax.random.split(folded, 2)
    length_all = NCH * SPAN
    query_draw = jax.random.truncated_normal(key_q, -6.0, 6.0, (LAYERS, SEQS, length_all, QH, HD), jnp.float32)
    key_draw = jax.random.truncated_normal(key_k, -6.0, 6.0, (LAYERS, SEQS, length_all, KVH, HD), jnp.float32)
    return (query_draw.reshape(LAYERS, SEQS, NCH, SPAN, QH, HD), key_draw.reshape(LAYERS, SEQS, NCH, SPAN, KVH, HD))


def draw_queries(key, part):
    return shared_draw(key)[0].astype(jnp.bfloat16)


def draw_keys(key, part):
    return shared_draw(key)[1].astype(jnp.bfloat16)


def place_ends(result, own_key, low, top_value):
    dims = result.shape
    spot = [jax.random.randint(jax.random.fold_in(own_key, axis), (), 0, dims[axis]) for axis in range(len(dims))]
    result = result.at[tuple(spot)].set(low)
    longest = dims.index(max(dims))
    spot[longest] = (spot[longest] + 1) % dims[longest]
    return result.at[tuple(spot)].set(top_value)


def levels(key, extent, pieces, smallest, high):
    def one(dim, shards_of):
        steps = jax.random.uniform(jax.random.fold_in(jax.random.fold_in(key, 6), dim), (shards_of,), jnp.float32, smallest / len(pieces), high / len(pieces))
        return jnp.repeat(jnp.exp(steps), extent[dim] // shards_of).reshape((-1,) + (1,) * (len(extent) - dim - 1))

    factor_of = one(*pieces[0])
    for cut in pieces[1:]:
        factor_of = factor_of * one(*cut)
    return factor_of


def centred(key, dims, deviation, limit, shards=(), dtype=jnp.bfloat16):
    level = levels(key, dims, shards, -0.22, 0.18) if shards else 1.0
    result = jax.random.normal(key, dims, jnp.float32) * deviation * level
    return jnp.minimum(jnp.maximum(result, -limit), limit).astype(dtype)


def setup_inputs(seed: int = 0) -> dict:
    key_of = jax.random.split(jax.random.key(seed), 6)
    return {
        "queries": draw_queries(jax.random.fold_in(key_of[5], 71), 0),
        "keys": draw_keys(jax.random.fold_in(key_of[5], 71), 0),
        "values": centred(key_of[2], (LAYERS, SEQS, NCH, SPAN, KVH, HD), 1.0, 6.0, ((0, 8), (3, 32))),
        "top_grad": centred(key_of[3], (SEQS, NCH, SPAN, QH, HD), 1.0, 6.0, ((2, 32),)),
        "head_live": place_ends((jax.random.randint(key_of[4], (QH,), 0, 8) < 7).astype(jnp.int32), jax.random.fold_in(key_of[4], 1), 0, 1),
    }


def head_backward(operands):
    query_h, key_h, value_h, grad_h = operands
    head_width = query_h.shape[-1]
    score_scale = head_width ** -0.5
    query_f = query_h.astype(jnp.float32)
    key_f = key_h.astype(jnp.float32)
    value_f = value_h.astype(jnp.float32)
    grad_f = grad_h.astype(jnp.float32)
    scores = jnp.einsum("sqd,skd->sqk", query_f, key_f) * score_scale
    length_all = scores.shape[1]
    rows_pos = lax.broadcasted_iota(jnp.int32, (length_all, length_all), 0)
    cols_pos = lax.broadcasted_iota(jnp.int32, (length_all, length_all), 1)
    scores = jnp.where((cols_pos <= rows_pos)[None], scores, -jnp.inf)
    prob_vals = jax.nn.softmax(scores, axis=-1)
    dprob_vals = jnp.einsum("sqd,skd->sqk", grad_f, value_f)
    delta = jnp.sum(prob_vals * dprob_vals, axis=-1, keepdims=True)
    dscore = (prob_vals * (dprob_vals - delta) * score_scale).astype(jnp.bfloat16)
    probs_half = prob_vals.astype(jnp.bfloat16)
    dscore = lax.optimization_barrier(dscore).astype(jnp.float32)
    probs_half = lax.optimization_barrier(probs_half).astype(jnp.float32)
    query_grad = jnp.einsum("sqk,skd->sqd", dscore, key_f)
    key_grad = jnp.einsum("sqk,sqd->skd", dscore, query_f)
    value_grad = jnp.einsum("sqk,sqd->skd", probs_half, grad_f)
    return query_grad, key_grad, value_grad


def reference(queries, keys, values, top_grad, head_live):
    layers, seqcount, spans, row_count, headcount, head_width = queries.shape
    kv_count = keys.shape[4]
    group_size = headcount // kv_count
    length_all = spans * row_count
    incoming = top_grad.reshape(seqcount, length_all, headcount, head_width)
    live_scale = head_live.astype(jnp.bfloat16)[None, None, :, None]
    input_list = [None] * layers
    key_list = [None] * layers
    value_list = [None] * layers
    for layer_idx in range(layers - 1, -1, -1):
        query_l = jnp.moveaxis(queries[layer_idx].reshape(seqcount, length_all, headcount, head_width), 2, 0)
        key_l = jnp.repeat(jnp.moveaxis(keys[layer_idx].reshape(seqcount, length_all, kv_count, head_width), 2, 0), group_size, axis=0)
        value_l = jnp.repeat(jnp.moveaxis(values[layer_idx].reshape(seqcount, length_all, kv_count, head_width), 2, 0), group_size, axis=0)
        grad_l = jnp.moveaxis(incoming * live_scale, 2, 0)
        query_grad, key_grad, value_grad = lax.map(head_backward, (query_l, key_l, value_l, grad_l))
        outgoing = (incoming.astype(jnp.float32) + jnp.moveaxis(query_grad, 0, 2)).astype(jnp.bfloat16)
        input_list[layer_idx] = outgoing.reshape(seqcount, spans, row_count, headcount, head_width)
        key_sum = key_grad.reshape(kv_count, group_size, seqcount, length_all, head_width).sum(axis=1)
        value_sum = value_grad.reshape(kv_count, group_size, seqcount, length_all, head_width).sum(axis=1)
        key_list[layer_idx] = jnp.moveaxis(key_sum, 0, 2).reshape(seqcount, spans, row_count, kv_count, head_width)
        value_list[layer_idx] = jnp.moveaxis(value_sum, 0, 2).reshape(seqcount, spans, row_count, kv_count, head_width)
        incoming = outgoing
    return jnp.stack(input_list), jnp.stack(key_list), jnp.stack(value_list)
```

```python
import functools
import math

import jax
import jax.numpy as jnp
from jax import lax
from jax.experimental import pallas as pl
from jax.experimental.pallas import tpu as pltpu
from jax.sharding import PartitionSpec as P

NY = 4
NX = 4
NC = 2
RUNS = (6, 2)


def place(y, x, core):
    return (y * NX + x) * NC + core


def ring_route(step, first):
    route = []
    for y in range(NY):
        for x in range(NX):
            for core in range(NC):
                if (core == 0) == first:
                    route.append((place(y, x, core), place(y, (x + step) % NX, core)))
                else:
                    route.append((place(y, x, core), place((y + step) % NY, x, core)))
    return route


def swap_cores(block):
    route = [
        (place(y, x, core), place(y, x, 1 - core))
        for y in range(NY)
        for x in range(NX)
        for core in range(NC)
    ]
    return lax.ppermute(block, "sp", route)


def swap_kinds(parts, layers):
    groups = [
        [z * NY * NX * NC + p * NC + core for z in range(layers) for core in range(NC)]
        for p in range(NY * NX)
    ]
    flat = parts.reshape((layers * NC,) + parts.shape[2:])
    return lax.all_to_all(
        flat, ("section", "sp"), 0, 0, tiled=True, axis_index_groups=groups
    ).reshape(parts.shape)


def gather_kind(pair):
    near = [lax.ppermute(pair, "sp", ring_route(d, True)) for d in (1, 2, 3)]
    lines = (jnp.stack([pair, near[0]]), jnp.stack(near[1:]))
    ahead = [lax.ppermute(half, "sp", ring_route(1, False)) for half in lines]
    back = [lax.ppermute(half, "sp", ring_route(-1, False)) for half in lines]
    far = [
        lax.ppermute(ahead[0], "sp", ring_route(1, False)),
        lax.ppermute(back[1], "sp", ring_route(-1, False)),
    ]
    mine = [*lines, *ahead, *far, *back]
    theirs = [swap_cores(part) for part in mine]
    return mine, theirs


def reduce_kind(keep, send):
    got = swap_cores(send)
    parts = [
        (keep[d].astype(jnp.float32) + got[d].astype(jnp.float32)).astype(jnp.bfloat16)
        for d in range(4)
    ]
    total = parts[0].astype(jnp.float32)
    for d in (1, 2, 3):
        total = total + lax.ppermute(parts[d], "sp", ring_route(-d, False)).astype(jnp.float32)
    parts = [total[d].astype(jnp.bfloat16) for d in range(4)]
    total = parts[0].astype(jnp.float32)
    for d in (1, 2, 3):
        total = total + lax.ppermute(parts[d], "sp", ring_route(-d, True)).astype(jnp.float32)
    return total.astype(jnp.bfloat16)


def fold_lanes(block, op):
    width = 128
    out = block[:, :width]
    for at in range(width, block.shape[1], width):
        out = op(out, block[:, at : at + width])
    return out


def dot(a, b, dims):
    return lax.dot_general(a, b, (dims, ((), ())), preferred_element_type=jnp.float32)


def layers_kernel(
    where_ref, live_ref, first_ref, q_ref, *refs
):
    mine_refs, their_refs = refs[:8], refs[8:16]
    out_ref, keep_ref, send_ref = refs[16:19]
    g_scr, do_scr, kv_scr, bias_scr, sc_scr, dp_scr, p_scr, ds_scr, part_scr = refs[19:]
    spans, span = 6, 512
    per = q_ref.shape[1] // spans
    width = q_ref.shape[2]
    scale = width**-0.5
    to_exp2 = scale * math.log2(math.e)
    core, my_y, my_x, my_sp = where_ref[0], where_ref[1], where_ref[2], where_ref[3]

    @pl.when(pl.program_id(0) == 0)
    def _():
        g_scr[...] = first_ref[...].reshape(g_scr.shape)
        row = lax.broadcasted_iota(jnp.int32, (per, span), 0)
        col = lax.broadcasted_iota(jnp.int32, (per, span), 1)
        key_y = (my_y - (col >> 7)) & 3
        key_x = (my_x - ((col >> 5) & 3)) & 3
        key_at = ((key_y * NX + key_x) * NC + ((col >> 4) & 1)) * 16 + (col & 15)
        row_at = my_sp * 16 + (row >> 3)
        bias_scr[...] = jnp.where(key_at <= row_at, 0.0, -jnp.inf).astype(jnp.float32)

    for at, (mine, theirs) in enumerate(zip(mine_refs, their_refs)):
        d, half = at // 2, pl.ds(2 * (at % 2), 2)
        for b in range(spans):
            kv_scr[core, b, d, half] = mine[:, 0, :, b].reshape(2, 32, width)
            kv_scr[1 - core, b, d, half] = theirs[:, 0, :, b].reshape(2, 32, width)
    do_scr[...] = (g_scr[...].astype(jnp.float32) * live_ref[...].astype(jnp.float32)).astype(
        jnp.bfloat16
    )

    def key_block(b):
        return kv_scr[0, b].reshape(span, width)

    def value_block(b):
        return jnp.swapaxes(kv_scr[1, b], 0, 1).reshape(span, width)

    for s in range(spans):
        rows = pl.ds(per * s, per)
        q_s = q_ref[0, rows, :]
        do_s = do_scr[rows, :]
        slot = s % 2
        top = None
        for b in range(s + 1):
            cols = pl.ds(span * b, span)
            sc = dot(q_s, key_block(b), ((1,), (1,)))
            if b == s:
                sc = sc + bias_scr[...]
            sc_scr[slot, :, cols] = sc
            here = fold_lanes(sc, jnp.maximum)
            top = here if top is None else jnp.maximum(top, here)
        top = jnp.max(top, axis=-1, keepdims=True)
        total = moment = None
        for b in range(s + 1):
            cols = pl.ds(span * b, span)
            dp = dot(do_s, value_block(b), ((1,), (1,)))
            p = jnp.exp2((sc_scr[slot, :, cols] - top) * to_exp2)
            sc_scr[slot, :, cols] = p
            dp_scr[slot, :, cols] = dp
            here, there = fold_lanes(p, jnp.add), fold_lanes(p * dp, jnp.add)
            total = here if total is None else total + here
            moment = there if moment is None else moment + there
        inverse = 1.0 / jnp.sum(total, axis=-1, keepdims=True)
        delta = jnp.sum(moment, axis=-1, keepdims=True) * inverse
        for b in range(s + 1):
            cols = pl.ds(span * b, span)
            p = sc_scr[slot, :, cols] * inverse
            p_scr[rows, cols] = p.astype(jnp.bfloat16)
            ds_scr[rows, cols] = (p * (dp_scr[slot, :, cols] - delta)).astype(jnp.bfloat16)
        dq = dot(
            ds_scr[rows, pl.ds(0, span * (s + 1))],
            kv_scr[0, pl.ds(0, s + 1)].reshape(span * (s + 1), width),
            ((1,), (0,)),
        )
        new = (g_scr[rows, :].astype(jnp.float32) + dq * scale).astype(jnp.bfloat16)
        out_ref[0, rows, :] = new
        g_scr[rows, :] = new

    q_t = q_ref[0].T
    do_t = do_scr[...].T
    for b in range(spans):
        cols = pl.ds(span * b, span)
        below = pl.ds(per * b, per * (spans - b))
        dk = dot(q_t[:, per * b :], ds_scr[below, cols], ((1,), (0,))) * scale
        dv = dot(do_t[:, per * b :], p_scr[below, cols], ((1,), (0,)))
        dk = dk.T.astype(jnp.bfloat16).reshape(4, 4, 32, width)
        dv = dv.T.astype(jnp.bfloat16).reshape(4, 4, 32, width)
        part_scr[core, b] = dk
        part_scr[1 - core, b] = jnp.swapaxes(dv, 0, 1)
    for b in range(spans):
        keep_ref[:, :, 0, :, b] = part_scr[0, b].reshape(4, 4, 2, 16, width)
        send_ref[:, :, 0, :, b] = part_scr[1, b].reshape(4, 4, 2, 16, width)


def run_layers(where, live, first, q, mine, theirs, top, count):
    rows, width = q.shape[1:]
    spans, short = mine[0].shape[3:5]
    length = spans * 512
    low = top - count + 1
    elements = rows * (length + 512) // 2
    kv_block = pl.BlockSpec(
        (2, 1, 2, spans, short, width), lambda i, at: (0, top - i, 0, 0, 0, 0)
    )
    part_block = pl.BlockSpec(
        (4, 4, 1, 2, spans, short, width), lambda i, at: (0, 0, count - 1 - i, 0, 0, 0, 0)
    )
    part_shape = jax.ShapeDtypeStruct((4, 4, count, 2, spans, short, width), jnp.bfloat16)
    whole = pl.BlockSpec((rows, width), lambda i, at: (0, 0))
    return pl.pallas_call(
        layers_kernel,
        grid_spec=pltpu.PrefetchScalarGridSpec(
        num_scalar_prefetch=1,
        grid=(count,),
        in_specs=[
            whole,
            whole if first.ndim == 2 else pl.BlockSpec((1, rows, width), lambda i, at: (top + 1, 0, 0)),
            pl.BlockSpec((1, rows, width), lambda i, at: (top - i, 0, 0)),
        ]
        + [kv_block] * 16,
        out_specs=[
            pl.BlockSpec((1, rows, width), lambda i, at: (top - i, 0, 0)),
            part_block,
            part_block,
        ],
        scratch_shapes=[
            pltpu.VMEM((rows, width), jnp.bfloat16),
            pltpu.VMEM((rows, width), jnp.bfloat16),
            pltpu.VMEM((2, spans, 4, 4, 32, width), jnp.bfloat16),
            pltpu.VMEM((rows // spans, 512), jnp.float32),
            pltpu.VMEM((2, rows // spans, length), jnp.float32),
            pltpu.VMEM((2, rows // spans, length), jnp.float32),
            pltpu.VMEM((rows, length), jnp.bfloat16),
            pltpu.VMEM((rows, length), jnp.bfloat16),
            pltpu.VMEM((2, spans, 4, 4, 32, width), jnp.bfloat16),
        ],
        ),
        out_shape=[
            jax.ShapeDtypeStruct(q.shape, jnp.bfloat16),
            part_shape,
            part_shape,
        ],
        compiler_params=pltpu.CompilerParams(
            dimension_semantics=("arbitrary",), vmem_limit_bytes=48 * 1024 * 1024
        ),
        cost_estimate=pl.CostEstimate(
            flops=count * elements * width * 2 * 5,
            bytes_accessed=count * 4 * 1024 * 1024,
            transcendentals=count * elements,
        ),
        input_output_aliases={} if first.ndim == 2 else {2: 0},
        name="layers_%d_%d" % (top, low),
    )(where, live, first, q, *mine, *theirs)


def body(queries, keys, values, top_grad, head_live):
    section = lax.axis_index("section")
    layers = lax.axis_size("section")
    sp = lax.axis_index("sp")
    core, x, y = sp % NC, (sp // NC) % NX, sp // (NC * NX)
    where = jnp.stack([core, y, x, sp]).astype(jnp.int32)
    _, seqs, spans, short, heads, width = queries.shape
    kv_heads = keys.shape[4]
    group = heads // kv_heads
    rows = spans * short * group

    def to_sections(parts, tail):
        return lax.all_to_all(parts, "section", split_axis=0, concat_axis=0, tiled=True).reshape(tail)

    kv = jnp.stack([keys[0], values[0]])
    kv = jnp.transpose(kv, (1, 4, 0, 2, 3, 5)).reshape(seqs * kv_heads, 2, spans, short, width)
    kv = swap_kinds(kv, layers)
    mine, theirs = gather_kind(kv)
    q = queries[0].reshape(seqs, spans, short, kv_heads, group, width)
    q = jnp.transpose(q, (0, 3, 1, 2, 4, 5)).reshape(seqs * kv_heads, rows, width)
    q, _ = lax.optimization_barrier((q, kv))
    q = to_sections(q, (layers, rows, width))

    seq, kv_head = section // kv_heads, section % kv_heads
    g = top_grad.reshape(seqs, spans, short, kv_heads, group, width)
    g = lax.dynamic_index_in_dim(g, seq, 0, keepdims=False)
    g = lax.dynamic_index_in_dim(g, kv_head, 2, keepdims=False).reshape(rows, width)
    live = lax.dynamic_index_in_dim(head_live.reshape(kv_heads, group), kv_head, 0, keepdims=False)
    live = jnp.broadcast_to(live.astype(jnp.bfloat16)[None, :, None], (spans * short, group, width))
    live = live.reshape(rows, width)

    top = layers - 1
    sums = []
    for count in RUNS:
        g, keep, send = run_layers(where, live, g, q, mine, theirs, top, count)
        sums.insert(0, reduce_kind(keep, send))
        top -= count

    out = to_sections(g, (seqs, kv_heads, spans, short, group, width))
    out = jnp.transpose(out, (0, 2, 3, 1, 4, 5)).reshape(seqs, spans, short, heads, width)
    total = swap_kinds(jnp.concatenate(sums), layers).astype(jnp.float32)
    total = total.reshape(seqs, kv_heads, 2, spans, short, width)
    total = jnp.transpose(total, (2, 0, 3, 4, 1, 5))
    return out[None], total[0][None], total[1][None]


def solution(mesh):
    return jax.shard_map(
        body,
        mesh=mesh,
        in_specs=(
            P("section", None, None, "sp", None, None),
            P("section", None, None, "sp", None, None),
            P("section", None, None, "sp", None, None),
            P(None, None, "sp", None, None),
            P(),
        ),
        out_specs=(
            P("section", None, None, "sp", None, None),
            P("section", None, None, "sp", None, None),
            P("section", None, None, "sp", None, None),
        ),
        check_vma=False,
    )
```
